32 devices in a mesh: grp: 4 (over x, core), blk: 2 (over y), set: 4 (over z).
Axes of the slice: x: 2, y: 2, z: 4, core: 2. Of those that a mesh axis runs over, the one named last changes fastest.
Arguments:
- queries: bfloat16 [4096, 384], P(('grp', 'blk', 'set')), may hold values from -8 to 8
- keys: bfloat16 [4096, 384], P(('grp', 'blk', 'set')), may hold values from -8 to 8
- values: bfloat16 [4096, 384], P(('grp', 'blk', 'set')), may hold values from -6 to 6
- valid: int32 [4096], P(('grp', 'blk', 'set')), may hold values 0 or 1
- offsets: int32 [2, 6], replicated, may hold values from 0 to 7, as said below
- w_out: bfloat16 [384, 768], replicated, may hold values from -0.3125 to 0.3125
Outputs:
- projected: bfloat16 [4096, 768], P(('grp', 'blk', 'set'))
The draws below stay inside these ranges and needn't reach their ends.
Inputs may be any that keep to these rules, and one draw needn't show every extreme that they name: offsets[0, h] lies in 0 to 1 and offsets[1, h] - offsets[0, h] is a multiple of 2 for every head h.
All inputs are finite; a program needn't handle non-finite values. No bound on the sum of `valid` on one device may be relied on, other than what follows from the above.
Results may differ from the reference program's by a relative error of at most 0.0015.
The reference program's roundings to bfloat16 on the way count: a program that leaves them out, or rounds other values in their place, can miss the bound.
Values may be sent and summed in bfloat16 or wider, within the bound.
A program may use at most 64 MiB of HBM per device.

```python
import math
import jax
import jax.numpy as jnp
from jax import lax

MODEL_WIDTH = 768
HEAD_COUNT = 6
HD = 64
ATT_WIDTH = 384
FIRST_SEGMENT = 512
TOKENS = 4096
SECOND_DILATION = 2
THIRD_DILATION = 8


def drawn_pair(key):
    base_key = jax.random.fold_in(key, 17)
    first_key, second_key = jax.random.split(base_key, 2)
    full_shape = (TOKENS, ATT_WIDTH)
    query_draw = jnp.clip(1.5 * jax.random.normal(first_key, full_shape, jnp.float32), -8.0, 8.0)
    key_draw = jnp.clip(1.5 * jax.random.normal(second_key, full_shape, jnp.float32), -8.0, 8.0)
    return (query_draw, key_draw)


def draw_queries(key, part):
    return drawn_pair(key)[0].astype(jnp.bfloat16)


def draw_keys(key, part):
    return drawn_pair(key)[1].astype(jnp.bfloat16)


def draw_offsets(key, part):
    base_key = jax.random.fold_in(key, 29)
    bottom_key, ceiling_key = jax.random.split(base_key)
    middle_shift = jax.random.randint(bottom_key, (HEAD_COUNT,), 0, SECOND_DILATION)
    outer_shift = middle_shift + SECOND_DILATION * jax.random.randint(ceiling_key, (HEAD_COUNT,), 0, THIRD_DILATION // SECOND_DILATION)
    return jnp.stack([middle_shift, outer_shift]).astype(jnp.int32)


def set_ends(drawn, own_key, low, high):
    longest = drawn.shape.index(max(drawn.shape))
    spots = []
    for shift in (0, 1):
        where = [jax.random.randint(jax.random.fold_in(own_key, axis), (), 0, length) for axis, length in enumerate(drawn.shape)]
        where[longest] = (where[longest] + shift) % drawn.shape[longest]
        spots.append(tuple(where))
    return drawn.at[spots[0]].set(low).at[spots[1]].set(high)


def level_of(key, shape, cuts, least, largest):
    def one(dim, parts):
        steps = jax.random.uniform(jax.random.fold_in(jax.random.fold_in(key, 6), dim), (parts,), jnp.float32, least / len(cuts), largest / len(cuts))
        return jnp.repeat(jnp.exp(steps), shape[dim] // parts).reshape((-1,) + (1,) * (len(shape) - dim - 1))

    loudness = one(*cuts[0])
    for cut in cuts[1:]:
        loudness = loudness * one(*cut)
    return loudness


def normal_values(own_key, extent, width, limit, cuts=(), kind=jnp.bfloat16):
    array = jax.random.normal(own_key, extent, jnp.float32) * width
    if len(cuts) > 0:
        array = level_of(own_key, extent, cuts, -0.22, 0.18) * array
    return jnp.clip(array, min=-limit, max=limit).astype(kind)


def setup_inputs(seed: int = 0) -> dict:
    streams_of = jax.random.split(jax.random.key(seed), 7)
    return {
        "queries": draw_queries(jax.random.fold_in(streams_of[6], 71), 0),
        "keys": draw_keys(jax.random.fold_in(streams_of[6], 71), 0),
        "values": normal_values(streams_of[2], (TOKENS, ATT_WIDTH), 1.0, 6.0, ((0, 32),)),
        "valid": set_ends((jax.random.randint(streams_of[3], (TOKENS,), 0, 4) < 3).astype(jnp.int32), jax.random.fold_in(streams_of[3], 1), 0, 1),
        "offsets": draw_offsets(jax.random.fold_in(streams_of[6], 71), 0),
        "w_out": normal_values(streams_of[5], (ATT_WIDTH, MODEL_WIDTH), ATT_WIDTH ** -0.5, 0.3125),
    }


def head_attend(query_head, key_head, value_head, key_allowed, self_slot, scaling):
    scores = lax.dot_general(query_head, key_head, (((1,), (1,)), ((), ())), preferred_element_type=jnp.float32) * scaling
    columns = jnp.arange(key_head.shape[0], dtype=jnp.int32)
    allowed = key_allowed[None, :] | (columns[None, :] == self_slot[:, None])
    scores = jnp.where(allowed, scores, jnp.float32(-1e+30))
    highest = lax.optimization_barrier(jnp.max(scores, axis=1, keepdims=True))
    weights = jnp.exp(scores - highest)
    totals = lax.optimization_barrier(jnp.sum(weights, axis=1))
    mixture = jnp.dot(weights.astype(jnp.bfloat16), value_head, preferred_element_type=jnp.float32) / totals[:, None]
    return (mixture, highest[:, 0] + jnp.log(totals))

def attend(queries, keys, values, key_allowed, self_slot):
    row_count = queries.shape[0]
    length = keys.shape[0]
    heads_query = queries.reshape(row_count, HEAD_COUNT, HD).transpose(1, 0, 2)
    heads_key = keys.reshape(length, HEAD_COUNT, HD).transpose(1, 0, 2)
    heads_value = values.reshape(length, HEAD_COUNT, HD).transpose(1, 0, 2)
    scaling = 1.0 / math.sqrt(HD)
    mixture, log_totals = lax.map(lambda packed: head_attend(packed[0], packed[1], packed[2], packed[3], self_slot, scaling), (heads_query, heads_key, heads_value, key_allowed.T))
    return (mixture.transpose(1, 0, 2).reshape(row_count, HEAD_COUNT * HD), log_totals.T)

def selector_table(shift_amount, cycle_length):
    return jnp.arange(cycle_length, dtype=jnp.int32)[:, None] == shift_amount[None, :]

def pick_rows(matrix, shift_amount, cycle_length):
    row_total = matrix.shape[0]
    selector = selector_table(shift_amount, cycle_length)
    blocks = matrix.reshape(row_total // cycle_length, cycle_length, HEAD_COUNT, HD)
    chosen = lax.optimization_barrier(jnp.sum(jnp.where(selector[None, :, :, None], blocks, jnp.zeros((), matrix.dtype)), axis=1))
    return chosen.reshape(row_total // cycle_length, HEAD_COUNT * HD)

def pick_flags(key_flags, shift_amount, cycle_length):
    row_total = key_flags.shape[0]
    selector = selector_table(shift_amount, cycle_length)
    blocks = key_flags.reshape(row_total // cycle_length, cycle_length)
    return lax.optimization_barrier(jnp.sum(jnp.where(selector[None, :, :], blocks[:, :, None], jnp.zeros((), key_flags.dtype)), axis=1))

def spread_back(mixture, log_totals, shift_amount, cycle_length):
    row_count = mixture.shape[0]
    selector = selector_table(shift_amount, cycle_length)
    wide = jnp.where(selector[None, :, :, None], mixture.reshape(row_count, 1, HEAD_COUNT, HD), jnp.float32(0.0))
    spread_totals = jnp.where(selector[None, :, :], log_totals[:, None, :], jnp.float32(0.0))
    present = jnp.broadcast_to(selector[None, :, :], (row_count, cycle_length, HEAD_COUNT))
    return (wide.reshape(row_count * cycle_length, HEAD_COUNT * HD), spread_totals.reshape(row_count * cycle_length, HEAD_COUNT), present.reshape(row_count * cycle_length, HEAD_COUNT))

def combine(levels):
    highest = levels[0][1]
    for entry in levels[1:]:
        highest = jnp.maximum(highest, jnp.where(entry[2], entry[1], highest))
    numerator = jnp.zeros(levels[0][0].shape, jnp.float32)
    denominator = jnp.zeros(levels[0][1].shape, jnp.float32)
    for entry in levels:
        scaled = jnp.where(entry[2], jnp.exp(entry[1] - highest), jnp.float32(0.0))
        expanded = jnp.broadcast_to(scaled[:, :, None], (scaled.shape[0], HEAD_COUNT, HD)).reshape(scaled.shape[0], HEAD_COUNT * HD)
        numerator = numerator + entry[0] * expanded
        denominator = denominator + scaled
    wide_denominator = jnp.broadcast_to(denominator[:, :, None], (denominator.shape[0], HEAD_COUNT, HD)).reshape(denominator.shape[0], HEAD_COUNT * HD)
    return numerator / wide_denominator

def segmented(queries, keys, values, key_allowed, segment):
    total_rows = queries.shape[0]
    pieces = total_rows // segment
    slot_index = jnp.arange(segment, dtype=jnp.int32)
    mixture, log_totals = lax.map(lambda packed: attend(packed[0], packed[1], packed[2], packed[3], slot_index), (queries.reshape(pieces, segment, HEAD_COUNT * HD), keys.reshape(pieces, segment, HEAD_COUNT * HD), values.reshape(pieces, segment, HEAD_COUNT * HD), key_allowed.reshape(pieces, segment, HEAD_COUNT)))
    return (mixture.reshape(total_rows, HEAD_COUNT * HD), log_totals.reshape(total_rows, HEAD_COUNT))

def reference(queries, keys, values, valid, offsets, w_out):
    total_rows = queries.shape[0]
    key_flags = valid.astype(jnp.float32)
    dense_allowed = jnp.broadcast_to((valid == 1)[:, None], (total_rows, HEAD_COUNT))
    dense_level = segmented(queries, keys, values, dense_allowed, FIRST_SEGMENT)
    levels = [(dense_level[0], dense_level[1], jnp.ones((total_rows, HEAD_COUNT), jnp.bool_))]
    for shift_amount, cycle_length in ((offsets[0], SECOND_DILATION), (offsets[1], THIRD_DILATION)):
        sparse_query = pick_rows(queries, shift_amount, cycle_length)
        sparse_key = pick_rows(keys, shift_amount, cycle_length)
        sparse_value = pick_rows(values, shift_amount, cycle_length)
        sparse_allowed = pick_flags(key_flags, shift_amount, cycle_length) > 0.5
        mixture, log_totals = segmented(sparse_query, sparse_key, sparse_value, sparse_allowed, FIRST_SEGMENT)
        levels.append(spread_back(mixture, log_totals, shift_amount, cycle_length))
    attention = combine(levels).astype(jnp.bfloat16)
    return jnp.dot(attention, w_out, preferred_element_type=jnp.float32).astype(jnp.bfloat16)
```

```python
import functools

import jax
import jax.numpy as jnp
from jax import lax
from jax.experimental import pallas as pl
from jax.experimental.pallas import tpu as pltpu
from jax.sharding import PartitionSpec as P

HEAD_COUNT = 6
HD = 64
LANES = 128
UNIT = 16
FLAG_STRIDE = 8
CHUNKS = HEAD_COUNT * HD // LANES
MESH = pl.DeviceIdType.MESH
NEG = -1e30


def units(count):
    return -(-count // UNIT)


def split_pow2(x, size):
    shift = size.bit_length() - 1
    return lax.shift_right_logical(x, shift), x & (size - 1)


class Plan:
    def __init__(self, grp, blk, n, rows):
        self.grp, self.blk, self.n, self.rows = grp, blk, n, rows
        self.period = grp * blk
        self.c3 = rows // self.period
        c2 = rows // blk
        self.counts = (self.c3, c2 - self.c3, rows - c2)
        self.units = tuple(units(c) for c in self.counts)
        self.sizes = tuple(u * UNIT for u in self.units)
        self.starts = (0, self.sizes[0], self.sizes[0] + self.sizes[1])
        self.total = sum(self.sizes)

    def source(self, t):
        a = t
        b = t - self.starts[1]
        c = t - self.starts[2]
        bv, bg = split_pow2(b, self.c3)
        cv, cg = split_pow2(c, self.c3)
        ck, cm = split_pow2(cv, self.grp)
        is_a = t < self.starts[1]
        is_b = t < self.starts[2]
        group = jnp.where(is_a, a, jnp.where(is_b, bg, cg))
        slot = jnp.where(is_a, 0, jnp.where(is_b, (bv + 1) * self.blk, cm * self.blk + ck + 1))
        local = jnp.where(is_a, a, jnp.where(is_b, b, c))
        count = jnp.where(is_a, self.counts[0], jnp.where(is_b, self.counts[1], self.counts[2]))
        return jnp.where(local < count, group * self.period, -(1 << 20)), slot


def kernel(
    plan, q_ref, k_ref, v_ref, valid_ref, offs_ref, w_ref, o_ref,
    buf_a, buf_b, buf_c, qs, zrecv, zsend, yrecv, ysend, xrecv, xsend, fsend,
):
    G, B, N = plan.grp, plan.blk, plan.n
    R = plan.total
    gi, bi, si = lax.axis_index("grp"), lax.axis_index("blk"), lax.axis_index("set")
    core = gi % 2
    partner = gi + 1 - 2 * core

    def peer_grp(step):
        return lax.rem(gi + 2 * step, G)

    barrier = pltpu.get_barrier_semaphore()

    def greet(g, b, s):
        pl.semaphore_signal(barrier, inc=1, device_id=(g, b, s), device_id_type=MESH)

    @pl.when(si > 0)
    def _():
        greet(gi, bi, si - 1)

    @pl.when(si < N - 1)
    def _():
        greet(gi, bi, si + 1)

    for step in range(1, B):
        greet(gi, lax.rem(bi + step, B), si)
    for step in range(1, G // 2):
        greet(peer_grp(step), bi, si)
    greet(partner, bi, si)

    lane = lax.broadcasted_iota(jnp.int32, (R, LANES), 1)
    base, slot = plan.source(lax.broadcasted_iota(jnp.int32, (R, plan.rows), 0))
    token = lax.broadcasted_iota(jnp.int32, (R, plan.rows), 1)
    valid_row = (valid_ref[...] > 0).astype(jnp.float32)
    flag_lane = lax.broadcasted_iota(jnp.int32, (UNIT, LANES), 1)
    flags = jnp.zeros((UNIT, LANES), jnp.float32)
    for c in range(CHUNKS):
        cols = slice(c * LANES, (c + 1) * LANES)
        packed = jnp.concatenate([q_ref[:, cols], k_ref[:, cols], v_ref[:, cols]], axis=1)
        moved = []
        for half in range(2):
            h = 2 * c + half
            hit = token == base + ((slot + offs_ref[1, h]) & (plan.period - 1))
            onehot = jnp.where(hit, jnp.float32(1), jnp.float32(0))
            moved.append(jnp.dot(onehot.astype(jnp.bfloat16), packed, preferred_element_type=jnp.float32))
            column = jnp.sum(onehot * valid_row, axis=1, keepdims=True)
            for u in range(R // UNIT):
                flags = jnp.where(
                    flag_lane == u * FLAG_STRIDE + h, column[u * UNIT:(u + 1) * UNIT, :], flags
                )
        for part in range(3):
            seg = slice(part * LANES, (part + 1) * LANES)
            got = jnp.where(lane < HD, moved[0][:, seg], moved[1][:, seg])
            if part == 0:
                qs[c] = (got * 0.125).astype(jnp.bfloat16)
                continue
            got = got.astype(jnp.bfloat16)
            at = c + (part - 1) * CHUNKS
            buf_a[0, 0, 0, at] = got[:plan.starts[1]]
            buf_b[0, 0, at] = got[plan.starts[1]:plan.starts[2]]
            buf_c[0, at] = got[plan.starts[2]:]
    buf_a[0, 0, 0, 2 * CHUNKS, 0:UNIT] = flags.astype(jnp.bfloat16)

    left_side = jnp.where(si > 0, 1, 0)
    right_side = jnp.where(si < N - 1, 1, 0)
    pl.semaphore_wait(barrier, left_side + right_side + (B - 1) + (G // 2 - 1) + 1)

    def zslot(part, r):
        return (buf_a.at[0, 0, r], buf_b.at[0, r], buf_c.at[r])[part]

    def zcopy(part, r, direction):
        to = (r + 1) % N if direction == 0 else (r - 1) % N
        near = si - 1 if direction == 0 else si + 1
        return pltpu.make_async_remote_copy(
            src_ref=zslot(part, r), dst_ref=zslot(part, to),
            send_sem=zsend.at[part, r, direction], recv_sem=zrecv.at[part, to],
            device_id=(gi, bi, near), device_id_type=MESH,
        )

    def ycopy(part, r, step):
        to = B - step

        def place(x):
            return buf_a.at[0, x, r] if part == 0 else buf_b.at[x, r]

        return pltpu.make_async_remote_copy(
            src_ref=place(0), dst_ref=place(to),
            send_sem=ysend.at[part, step, r], recv_sem=yrecv.at[part, to, r],
            device_id=(gi, lax.rem(bi + step, B), si), device_id_type=MESH,
        )

    def xcopy(y, r, step):
        to = (2 * (G // 2 - step)) % G
        return pltpu.make_async_remote_copy(
            src_ref=buf_a.at[0, y, r], dst_ref=buf_a.at[to, y, r],
            send_sem=xsend.at[step, y, r], recv_sem=xrecv.at[to, y, r],
            device_id=(peer_grp(step), bi, si), device_id_type=MESH,
        )

    def fcopy(x, y, r):
        return pltpu.make_async_remote_copy(
            src_ref=buf_a.at[x, y, r], dst_ref=buf_a.at[x + 1, y, r],
            send_sem=fsend.at[x, y, r], recv_sem=xrecv.at[x + 1, y, r],
            device_id=(partner, bi, si), device_id_type=MESH,
        )

    def spread_grp(y, r):
        for step in range(1, G // 2):
            xcopy(y, r, step).start()
        fcopy(0, y, r).start()

    def spread_blk(part, r):
        for step in range(1, B):
            ycopy(part, r, step).start()

    def own_z(part):
        @pl.when(si > 0)
        def _():
            zcopy(part, 0, 0).start()

        @pl.when(si < N - 1)
        def _():
            zcopy(part, 0, 1).start()

    def arrive(part, r):
        pltpu.make_async_copy(zslot(part, r), zslot(part, r), zrecv.at[part, r]).wait()

    def take(part, d):
        @pl.when(si + d <= N - 1)
        def _():
            arrive(part, d)

            @pl.when(si > 0)
            def _():
                zcopy(part, d, 0).start()

            if part < 2:
                spread_blk(part, d)
            if part == 0:
                spread_grp(0, d)

        @pl.when(si - d >= 0)
        def _():
            arrive(part, N - d)

            @pl.when(si < N - 1)
            def _():
                zcopy(part, N - d, 1).start()

            if part < 2:
                spread_blk(part, N - d)
            if part == 0:
                spread_grp(0, N - d)

    own_z(0)
    spread_blk(0, 0)
    spread_grp(0, 0)
    own_z(1)
    spread_blk(1, 0)
    for d in range(1, N):
        take(0, d)
        take(1, d)
        if d == 1:
            own_z(2)
    for r in range(N):
        for y in range(1, B):
            ref = buf_a.at[0, y, r]
            pltpu.make_async_copy(ref, ref, yrecv.at[0, y, r]).wait()
            spread_grp(y, r)
    if N > 1:
        take(2, 1)
    for r in range(N):
        for y in range(B):
            for step in range(1, G // 2):
                ref = buf_a.at[2 * step, y, r]
                pltpu.make_async_copy(ref, ref, xrecv.at[2 * step, y, r]).wait()
                fcopy(2 * step, y, r).start()
    for d in range(2, N):
        take(2, d)

    head_pick = lax.broadcasted_iota(jnp.int32, (FLAG_STRIDE, LANES), 1) & (FLAG_STRIDE - 1)
    head_pick = head_pick == lax.broadcasted_iota(jnp.int32, (FLAG_STRIDE, LANES), 0)
    head_pick = jnp.where(head_pick, jnp.float32(1), jnp.float32(0)).astype(jnp.bfloat16)

    def gather(level, at):
        pieces = []
        for u in range(plan.units[0]):
            rows = slice(u * UNIT, (u + 1) * UNIT)
            part = (buf_a[0, 0, :, at, rows], buf_a[0, :, :, at, rows], buf_a[:, :, :, at, rows])[level]
            pieces.append(part.reshape(-1, LANES))
        if level < 2:
            for u in range(plan.units[1]):
                rows = slice(u * UNIT, (u + 1) * UNIT)
                part = buf_b[0, :, at, rows] if level == 0 else buf_b[:, :, at, rows]
                pieces.append(part.reshape(-1, LANES))
        if level == 0:
            for u in range(plan.units[2]):
                pieces.append(buf_c[:, at, u * UNIT:(u + 1) * UNIT].reshape(-1, LANES))
        return pieces[0] if len(pieces) == 1 else jnp.concatenate(pieces, axis=0)

    def level_attend(level):
        M = (R, plan.starts[2], plan.starts[1])[level]
        tiles = M // UNIT
        devices = (N, B * N, G * B * N)[level]
        per_unit = devices * UNIT
        rows = slice(0, UNIT)
        at = 2 * CHUNKS
        tall = (buf_a[0, 0, :, at, rows], buf_a[0, :, :, at, rows], buf_a[:, :, :, at, rows])[level]
        tall = tall.reshape(per_unit, LANES).astype(jnp.float32)
        unit_lane = lax.broadcasted_iota(jnp.int32, (per_unit, LANES), 1) // FLAG_STRIDE
        tall = [jnp.where(unit_lane == u, tall, 0.0).astype(jnp.bfloat16) for u in range(tiles)]
        tall = tall[0] if tiles == 1 else jnp.concatenate(tall, axis=0)
        ok = lax.dot_general(
            head_pick, tall, (((1,), (1,)), ((), ())), preferred_element_type=jnp.float32
        )
        keys = per_unit * tiles
        t = lax.broadcasted_iota(jnp.int32, (M, keys), 0)
        own = lax.broadcasted_iota(jnp.int32, (M, keys), 1) == (t // UNIT) * per_unit + (t % UNIT)
        half_lane = lax.broadcasted_iota(jnp.int32, (M, LANES), 1) < HD
        results = []
        for c in range(CHUNKS):
            q = qs[c, 0:M]
            zero = jnp.zeros_like(q)
            both = jnp.concatenate([jnp.where(half_lane, q, zero), jnp.where(half_lane, zero, q)], axis=0)
            scores = lax.dot_general(
                both, gather(level, c), (((1,), (1,)), ((), ())), preferred_element_type=jnp.float32
            )
            values = gather(level, CHUNKS + c)
            probs, tops, totals = [], [], []
            for half in range(2):
                h = 2 * c + half
                s = jnp.where(own | (ok[h:h + 1, :] > 0.5), scores[half * M:(half + 1) * M], NEG)
                top = jnp.max(s, axis=1, keepdims=True)
                weight = jnp.exp(s - top)
                totals.append(jnp.sum(weight, axis=1, keepdims=True))
                tops.append(top)
                probs.append(weight.astype(jnp.bfloat16))
            mixed = jnp.dot(jnp.concatenate(probs, axis=0), values, preferred_element_type=jnp.float32)
            mixture = jnp.where(half_lane, mixed[:M] / totals[0], mixed[M:] / totals[1])
            lse = jnp.where(half_lane, tops[0] + jnp.log(totals[0]), tops[1] + jnp.log(totals[1]))
            results.append((mixture, lse))
        return results

    first = level_attend(0)
    for r in range(N):
        for y in range(1, B):
            ref = buf_b.at[y, r]
            pltpu.make_async_copy(ref, ref, yrecv.at[1, y, r]).wait()
    second = level_attend(1)
    for r in range(N):
        for y in range(B):
            for x in range(1, G, 2):
                ref = buf_a.at[x, y, r]
                pltpu.make_async_copy(ref, ref, xrecv.at[x, y, r]).wait()
    third = level_attend(2)

    a_end, b_end = plan.starts[1], plan.starts[2]

    def combine(levels):
        top = functools.reduce(jnp.maximum, [lse for _, lse in levels])
        shares = [jnp.exp(lse - top) for _, lse in levels]
        return sum(s * o for s, (o, _) in zip(shares, levels)) / sum(shares)

    base, slot = plan.source(lax.broadcasted_iota(jnp.int32, (plan.rows, R), 1))
    token = lax.broadcasted_iota(jnp.int32, (plan.rows, R), 0)
    out_lane = lax.broadcasted_iota(jnp.int32, (plan.rows, LANES), 1)
    attention = []
    for c in range(CHUNKS):
        (o1, l1), (o2, l2), (o3, l3) = first[c], second[c], third[c]
        mixed = jnp.concatenate(
            [
                combine([(o1[:a_end], l1[:a_end]), (o2[:a_end], l2[:a_end]), (o3, l3)]),
                combine([(o1[a_end:b_end], l1[a_end:b_end]), (o2[a_end:], l2[a_end:])]),
                o1[b_end:],
            ],
            axis=0,
        ).astype(jnp.bfloat16)
        back = []
        for half in range(2):
            hit = token == base + ((slot + offs_ref[1, 2 * c + half]) & (plan.period - 1))
            onehot = jnp.where(hit, jnp.float32(1), jnp.float32(0)).astype(jnp.bfloat16)
            back.append(jnp.dot(onehot, mixed, preferred_element_type=jnp.float32))
        attention.append(jnp.where(out_lane < HD, back[0], back[1]).astype(jnp.bfloat16))
    attention = jnp.concatenate(attention, axis=1)
    o_ref[...] = jnp.dot(attention, w_ref[...], preferred_element_type=jnp.float32).astype(o_ref.dtype)

    for part in range(3):
        for r in range(N):
            goes_left = si > 0 if r == 0 else (si > 0) & (si + r <= N - 1)
            goes_right = si < N - 1 if r == 0 else (si < N - 1) & (si + r > N - 1)

            @pl.when(goes_left)
            def _():
                zcopy(part, r, 0).wait_send()

            @pl.when(goes_right)
            def _():
                zcopy(part, r, 1).wait_send()

            if part < 2:
                for step in range(1, B):
                    ycopy(part, r, step).wait_send()
            if part == 0:
                for y in range(B):
                    for step in range(1, G // 2):
                        xcopy(y, r, step).wait_send()
                    for x in range(0, G, 2):
                        fcopy(x, y, r).wait_send()


def solution(mesh):
    G, B, N = mesh.shape["grp"], mesh.shape["blk"], mesh.shape["set"]

    def per_device(queries, keys, values, valid, offsets, w_out):
        rows, width = queries.shape
        plan = Plan(G, B, N, rows)
        vmem = pl.BlockSpec(memory_space=pltpu.VMEM)
        smem = pl.BlockSpec(memory_space=pltpu.SMEM)
        dma = pltpu.SemaphoreType.DMA
        ra, rb, rc = plan.sizes
        return pl.pallas_call(
            functools.partial(kernel, plan),
            out_shape=jax.ShapeDtypeStruct((rows, w_out.shape[1]), jnp.bfloat16),
            in_specs=[vmem, vmem, vmem, vmem, smem, vmem],
            out_specs=vmem,
            scratch_shapes=[
                pltpu.VMEM((G, B, N, 2 * CHUNKS + 1, ra, LANES), jnp.bfloat16),
                pltpu.VMEM((B, N, 2 * CHUNKS, rb, LANES), jnp.bfloat16),
                pltpu.VMEM((N, 2 * CHUNKS, rc, LANES), jnp.bfloat16),
                pltpu.VMEM((CHUNKS, plan.total, LANES), jnp.bfloat16),
                dma((3, N)),
                dma((3, N, 2)),
                dma((2, B, N)),
                dma((2, B, N)),
                dma((G, B, N)),
                dma((G // 2, B, N)),
                dma((G, B, N)),
            ],
            compiler_params=pltpu.CompilerParams(
                collective_id=0, has_side_effects=True, vmem_limit_bytes=60 * 1024 * 1024
            ),
        )(queries, keys, values, valid.reshape(1, rows), offsets, w_out)

    rows_spec = P(("grp", "blk", "set"), None)
    return jax.shard_map(
        per_device,
        mesh=mesh,
        in_specs=(rows_spec, rows_spec, rows_spec, P(("grp", "blk", "set")), P(), P()),
        out_specs=rows_spec,
        check_vma=False,
    )
```

```python
import functools

import jax
import jax.numpy as jnp
from jax import lax
from jax.experimental import pallas as pl
from jax.experimental.pallas import tpu as pltpu
from jax.sharding import PartitionSpec as P

HEAD_COUNT = 6
HD = 64
LANES = 128
UNIT = 16
FLAG_STRIDE = 8
CHUNKS = HEAD_COUNT * HD // LANES
MESH = pl.DeviceIdType.MESH
NEG = -1e30
FLAG_SPOT = 2 * CHUNKS - 2


def spot(at):
    return at if at < FLAG_SPOT else at + 1


def units(count):
    return -(-count // UNIT)


def split_pow2(x, size):
    shift = size.bit_length() - 1
    return lax.shift_right_logical(x, shift), x & (size - 1)


class Plan:
    def __init__(self, grp, blk, n, rows):
        self.grp, self.blk, self.n, self.rows = grp, blk, n, rows
        self.period = grp * blk
        self.c3 = rows // self.period
        c2 = rows // blk
        self.counts = (self.c3, c2 - self.c3, rows - c2)
        self.units = tuple(units(c) for c in self.counts)
        self.sizes = tuple(u * UNIT for u in self.units)
        self.starts = (0, self.sizes[0], self.sizes[0] + self.sizes[1])
        self.total = sum(self.sizes)

    def source(self, t):
        a = t
        b = t - self.starts[1]
        c = t - self.starts[2]
        bv, bg = split_pow2(b, self.c3)
        cv, cg = split_pow2(c, self.c3)
        ck, cm = split_pow2(cv, self.grp)
        is_a = t < self.starts[1]
        is_b = t < self.starts[2]
        group = jnp.where(is_a, a, jnp.where(is_b, bg, cg))
        slot = jnp.where(is_a, 0, jnp.where(is_b, (bv + 1) * self.blk, cm * self.blk + ck + 1))
        local = jnp.where(is_a, a, jnp.where(is_b, b, c))
        count = jnp.where(is_a, self.counts[0], jnp.where(is_b, self.counts[1], self.counts[2]))
        return jnp.where(local < count, group * self.period, -(1 << 20)), slot


def kernel(
    plan, q_ref, k_ref, v_ref, valid_ref, offs_ref, o_ref,
    buf_a, buf_b, buf_c, qs, qdel, mixes, lses, comb, cdel,
    zrecv, zsend, yrecv, ysend, xrecv, xsend, fsend, dsend, drecv,
):
    G, B, N = plan.grp, plan.blk, plan.n
    R = plan.total
    gi, bi, si = lax.axis_index("grp"), lax.axis_index("blk"), lax.axis_index("set")
    core = gi % 2
    partner = gi + 1 - 2 * core
    is_first, is_last = si == 0, si == N - 1
    is_end = is_first | is_last
    is_helper = (si == 1) | (si == N - 2)
    helper_of_end = jnp.where(is_first, 1, N - 2)
    end_of_helper = jnp.where(si == 1, 0, N - 1)

    def cases(condition, action):
        pl.when(condition)(lambda: action(True))
        pl.when(jnp.logical_not(condition))(lambda: action(False))

    def peer_grp(step):
        return lax.rem(gi + 2 * step, G)

    barrier = pltpu.get_barrier_semaphore()

    def greet(g, b, s):
        pl.semaphore_signal(barrier, inc=1, device_id=(g, b, s), device_id_type=MESH)

    @pl.when(si > 0)
    def _():
        greet(gi, bi, si - 1)

    @pl.when(si < N - 1)
    def _():
        greet(gi, bi, si + 1)

    for step in range(1, B):
        greet(gi, lax.rem(bi + step, B), si)
    for step in range(1, G // 2):
        greet(peer_grp(step), bi, si)
    greet(partner, bi, si)

    lane = lax.broadcasted_iota(jnp.int32, (R, LANES), 1)
    base, slot = plan.source(lax.broadcasted_iota(jnp.int32, (R, plan.rows), 0))
    token = lax.broadcasted_iota(jnp.int32, (R, plan.rows), 1)
    valid_row = (valid_ref[...] > 0).astype(jnp.float32)
    flag_lane = lax.broadcasted_iota(jnp.int32, (UNIT, LANES), 1)
    flags = jnp.zeros((UNIT, LANES), jnp.float32)
    for c in range(CHUNKS):
        cols = slice(c * LANES, (c + 1) * LANES)
        packed = jnp.concatenate([q_ref[:, cols], k_ref[:, cols], v_ref[:, cols]], axis=1)
        moved = []
        for half in range(2):
            h = 2 * c + half
            hit = token == base + ((slot + offs_ref[1, h]) & (plan.period - 1))
            onehot = jnp.where(hit, jnp.float32(1), jnp.float32(0))
            moved.append(jnp.dot(onehot.astype(jnp.bfloat16), packed, preferred_element_type=jnp.float32))
            column = jnp.sum(onehot * valid_row, axis=1, keepdims=True)
            for u in range(R // UNIT):
                flags = jnp.where(
                    flag_lane == u * FLAG_STRIDE + h, column[u * UNIT:(u + 1) * UNIT, :], flags
                )
        for part in range(3):
            seg = slice(part * LANES, (part + 1) * LANES)
            got = jnp.where(lane < HD, moved[0][:, seg], moved[1][:, seg])
            if part == 0:
                qs[c] = (got * 0.125).astype(jnp.bfloat16)
                continue
            got = got.astype(jnp.bfloat16)
            at = 2 * c + part - 1
            buf_a[0, 0, 0, spot(at)] = got[:plan.starts[1]]
            buf_b[0, 0, at] = got[plan.starts[1]:plan.starts[2]]
            buf_c[0, at] = got[plan.starts[2]:]
    buf_a[0, 0, 0, FLAG_SPOT, 0:UNIT] = flags.astype(jnp.bfloat16)

    left_side = jnp.where(si > 0, 1, 0)
    right_side = jnp.where(si < N - 1, 1, 0)
    pl.semaphore_wait(barrier, left_side + right_side + (B - 1) + (G // 2 - 1) + 1)

    def width(part, short):
        full = 2 * CHUNKS + (part == 0)
        return pl.ds(0, full - 2 if short else full)

    def zslot(part, r, short):
        w = width(part, short)
        return (buf_a.at[0, 0], buf_b.at[0], buf_c)[part].at[r, w]

    def zcopy(part, r, direction, short):
        to = (r + 1) % N if direction == 0 else (r - 1) % N
        near = si - 1 if direction == 0 else si + 1
        return pltpu.make_async_remote_copy(
            src_ref=zslot(part, r, short), dst_ref=zslot(part, to, short),
            send_sem=zsend.at[part, r, direction], recv_sem=zrecv.at[part, to],
            device_id=(gi, bi, near), device_id_type=MESH,
        )

    def to_near(part, r, direction, method):
        near_end = si == 1 if direction == 0 else si == N - 2
        cases(near_end, lambda short: getattr(zcopy(part, r, direction, short), method)())

    def yplace(part, x, r, short):
        w = width(part, short)
        return buf_a.at[0, x, r, w] if part == 0 else buf_b.at[x, r, w]

    def ycopy(part, r, step, short):
        to = B - step
        return pltpu.make_async_remote_copy(
            src_ref=yplace(part, 0, r, short), dst_ref=yplace(part, to, r, short),
            send_sem=ysend.at[part, step, r], recv_sem=yrecv.at[part, to, r],
            device_id=(gi, lax.rem(bi + step, B), si), device_id_type=MESH,
        )

    def xplace(x, y, r, short):
        return buf_a.at[x, y, r, width(0, short)]

    def xcopy(y, r, step, short):
        to = (2 * (G // 2 - step)) % G
        return pltpu.make_async_remote_copy(
            src_ref=xplace(0, y, r, short), dst_ref=xplace(to, y, r, short),
            send_sem=xsend.at[step, y, r], recv_sem=xrecv.at[to, y, r],
            device_id=(peer_grp(step), bi, si), device_id_type=MESH,
        )

    def fcopy(x, y, r, short):
        return pltpu.make_async_remote_copy(
            src_ref=xplace(x, y, r, short), dst_ref=xplace(x + 1, y, r, short),
            send_sem=fsend.at[x, y, r], recv_sem=xrecv.at[x + 1, y, r],
            device_id=(partner, bi, si), device_id_type=MESH,
        )

    def qcopy():
        return pltpu.make_async_remote_copy(
            src_ref=qs.at[CHUNKS - 1], dst_ref=qdel, send_sem=dsend.at[0], recv_sem=drecv.at[0],
            device_id=(gi, bi, helper_of_end), device_id_type=MESH,
        )

    def backcopy():
        return pltpu.make_async_remote_copy(
            src_ref=cdel, dst_ref=comb.at[CHUNKS - 1], send_sem=dsend.at[1], recv_sem=drecv.at[1],
            device_id=(gi, bi, end_of_helper), device_id_type=MESH,
        )

    def wait_for(ref, sem):
        pltpu.make_async_copy(ref, ref, sem).wait()

    def spread_grp(y, r, short):
        for step in range(1, G // 2):
            xcopy(y, r, step, short).start()
        fcopy(0, y, r, short).start()

    def spread_blk(part, r, short):
        for step in range(1, B):
            ycopy(part, r, step, short).start()

    def spread(part, r):
        def action(short):
            if part < 2:
                spread_blk(part, r, short)
            if part == 0:
                spread_grp(0, r, short)

        cases(is_end, action)

    def own_z(part):
        pl.when(si > 0)(lambda: to_near(part, 0, 0, "start"))
        pl.when(si < N - 1)(lambda: to_near(part, 0, 1, "start"))

    def arrive(part, r):
        cases(is_end, lambda short: wait_for(zslot(part, r, short), zrecv.at[part, r]))

    def take(part, d):
        @pl.when(si + d <= N - 1)
        def _():
            arrive(part, d)
            pl.when(si > 0)(lambda: to_near(part, d, 0, "start"))
            if part < 2:
                spread(part, d)

        @pl.when(si - d >= 0)
        def _():
            arrive(part, N - d)
            pl.when(si < N - 1)(lambda: to_near(part, N - d, 1, "start"))
            if part < 2:
                spread(part, N - d)

    own_z(0)
    spread(0, 0)
    own_z(1)
    spread(1, 0)
    pl.when(is_end)(lambda: qcopy().start())
    for d in range(1, N):
        take(0, d)
        if d == 2:
            own_z(2)
        take(1, d)

    def relay_y(short):
        for r in range(N):
            for y in range(1, B):
                wait_for(yplace(0, y, r, short), yrecv.at[0, y, r])
                spread_grp(y, r, short)

    def relay_x(short):
        for r in range(N):
            for y in range(B):
                for step in range(1, G // 2):
                    wait_for(xplace(2 * step, y, r, short), xrecv.at[2 * step, y, r])
                    fcopy(2 * step, y, r, short).start()

    def last_x(short):
        for r in range(N):
            for y in range(B):
                for x in range(1, G, 2):
                    wait_for(xplace(x, y, r, short), xrecv.at[x, y, r])

    def last_y(short):
        for r in range(N):
            for y in range(1, B):
                wait_for(yplace(1, y, r, short), yrecv.at[1, y, r])

    cases(is_end, relay_y)
    take(2, 1)
    cases(is_end, relay_x)
    for d in range(2, N - 1):
        take(2, d)

    head_pick = lax.broadcasted_iota(jnp.int32, (FLAG_STRIDE, LANES), 1) & (FLAG_STRIDE - 1)
    head_pick = head_pick == lax.broadcasted_iota(jnp.int32, (FLAG_STRIDE, LANES), 0)
    head_pick = jnp.where(head_pick, jnp.float32(1), jnp.float32(0)).astype(jnp.bfloat16)

    def gather(level, at):
        pieces = []
        for u in range(plan.units[0]):
            rows = slice(u * UNIT, (u + 1) * UNIT)
            at_a = spot(at)
            part = (buf_a[0, 0, :, at_a, rows], buf_a[0, :, :, at_a, rows], buf_a[:, :, :, at_a, rows])[level]
            pieces.append(part.reshape(-1, LANES))
        if level < 2:
            for u in range(plan.units[1]):
                rows = slice(u * UNIT, (u + 1) * UNIT)
                part = buf_b[0, :, at, rows] if level == 0 else buf_b[:, :, at, rows]
                pieces.append(part.reshape(-1, LANES))
        if level == 0:
            for u in range(plan.units[2]):
                pieces.append(buf_c[:, at, u * UNIT:(u + 1) * UNIT].reshape(-1, LANES))
        return pieces[0] if len(pieces) == 1 else jnp.concatenate(pieces, axis=0)

    def level_attend(level):
        M = (R, plan.starts[2], plan.starts[1])[level]
        tiles = M // UNIT
        devices = (N, B * N, G * B * N)[level]
        per_unit = devices * UNIT
        rows = slice(0, UNIT)
        at = FLAG_SPOT
        tall = (buf_a[0, 0, :, at, rows], buf_a[0, :, :, at, rows], buf_a[:, :, :, at, rows])[level]
        tall = tall.reshape(per_unit, LANES).astype(jnp.float32)
        unit_lane = lax.broadcasted_iota(jnp.int32, (per_unit, LANES), 1) // FLAG_STRIDE
        tall = [jnp.where(unit_lane == u, tall, 0.0).astype(jnp.bfloat16) for u in range(tiles)]
        tall = tall[0] if tiles == 1 else jnp.concatenate(tall, axis=0)
        ok = lax.dot_general(
            head_pick, tall, (((1,), (1,)), ((), ())), preferred_element_type=jnp.float32
        )
        keys = per_unit * tiles
        t = lax.broadcasted_iota(jnp.int32, (M, keys), 0)
        key = lax.broadcasted_iota(jnp.int32, (M, keys), 1)
        home = (t // UNIT) * per_unit + (t % UNIT)
        half_lane = lax.broadcasted_iota(jnp.int32, (M, LANES), 1) < HD

        def job(index):
            c = min(index, CHUNKS - 1)
            q = qs[c, 0:M] if index < CHUNKS else qdel[0:M]
            own = key == (home if index < CHUNKS else home + end_slot * UNIT)
            zero = jnp.zeros_like(q)
            both = jnp.concatenate([jnp.where(half_lane, q, zero), jnp.where(half_lane, zero, q)], axis=0)
            scores = lax.dot_general(
                both, gather(level, 2 * c), (((1,), (1,)), ((), ())), preferred_element_type=jnp.float32
            )
            values = gather(level, 2 * c + 1)
            probs, tops, totals = [], [], []
            for half in range(2):
                h = 2 * c + half
                s = jnp.where(own | (ok[h:h + 1, :] > 0.5), scores[half * M:(half + 1) * M], NEG)
                top = jnp.max(s, axis=1, keepdims=True)
                weight = jnp.exp(s - top)
                totals.append(jnp.sum(weight, axis=1, keepdims=True))
                tops.append(top)
                probs.append(weight.astype(jnp.bfloat16))
            mixed = jnp.dot(jnp.concatenate(probs, axis=0), values, preferred_element_type=jnp.float32)
            mixes[level, index, 0:M] = jnp.where(half_lane, mixed[:M] / totals[0], mixed[M:] / totals[1])
            lses[level, index, 0:M] = jnp.where(
                half_lane, tops[0] + jnp.log(totals[0]), tops[1] + jnp.log(totals[1])
            )

        return job

    a_end, b_end = plan.starts[1], plan.starts[2]

    def combine(levels):
        top = functools.reduce(jnp.maximum, [lse for _, lse in levels])
        shares = [jnp.exp(lse - top) for _, lse in levels]
        return sum(s * o for s, (o, _) in zip(shares, levels)) / sum(shares)

    end_slot = jnp.where(si == 1, N - 1, 1)

    def level_jobs(level):
        job = level_attend(level)
        pl.when(is_helper)(lambda: job(CHUNKS))
        if level == 1:
            @pl.when(is_helper)
            def _():
                cdel[...] = merged(CHUNKS)
                backcopy().start()
        for c in range(CHUNKS - 1):
            job(c)
        pl.when(jnp.logical_not(is_end))(lambda: job(CHUNKS - 1))

    def merged(index):
        o1, o2, o3 = (mixes.at[level, index] for level in range(3))
        l1, l2, l3 = (lses.at[level, index] for level in range(3))
        a, b, c = slice(0, a_end), slice(a_end, b_end), slice(b_end, R)
        return jnp.concatenate(
            [
                combine([(o1[a], l1[a]), (o2[a], l2[a]), (o3[a], l3[a])]),
                combine([(o1[b], l1[b]), (o2[b], l2[b])]),
                o1[c],
            ],
            axis=0,
        ).astype(jnp.bfloat16)

    cases(is_end, last_x)
    pl.when(is_helper)(lambda: wait_for(qdel, drecv.at[0]))
    level_jobs(2)
    take(2, N - 1)
    level_jobs(0)
    cases(is_end, last_y)
    level_jobs(1)

    for c in range(CHUNKS - 1):
        comb[c] = merged(c)

    @pl.when(jnp.logical_not(is_end))
    def _():
        comb[CHUNKS - 1] = merged(CHUNKS - 1)

    pl.when(is_end)(lambda: wait_for(comb.at[CHUNKS - 1], drecv.at[1]))

    base, slot = plan.source(lax.broadcasted_iota(jnp.int32, (plan.rows, R), 1))
    token = lax.broadcasted_iota(jnp.int32, (plan.rows, R), 0)
    out_lane = lax.broadcasted_iota(jnp.int32, (plan.rows, LANES), 1)
    for c in range(CHUNKS):
        mixed = comb[c]
        back = []
        for half in range(2):
            hit = token == base + ((slot + offs_ref[1, 2 * c + half]) & (plan.period - 1))
            onehot = jnp.where(hit, jnp.float32(1), jnp.float32(0)).astype(jnp.bfloat16)
            back.append(jnp.dot(onehot, mixed, preferred_element_type=jnp.float32))
        o_ref[:, c * LANES:(c + 1) * LANES] = jnp.where(out_lane < HD, back[0], back[1]).astype(o_ref.dtype)

    def sent(short):
        for r in range(N):
            for step in range(1, B):
                ycopy(0, r, step, short).wait_send()
                ycopy(1, r, step, short).wait_send()
            for y in range(B):
                for step in range(1, G // 2):
                    xcopy(y, r, step, short).wait_send()
                for x in range(0, G, 2):
                    fcopy(x, y, r, short).wait_send()

    cases(is_end, sent)
    pl.when(is_end)(lambda: qcopy().wait_send())
    pl.when(is_helper)(lambda: backcopy().wait_send())
    for part in range(3):
        for r in range(N):
            goes_left = si > 0 if r == 0 else (si > 0) & (si + r <= N - 1)
            goes_right = si < N - 1 if r == 0 else (si < N - 1) & (si + r > N - 1)
            pl.when(goes_left)(lambda: to_near(part, r, 0, "wait_send"))
            pl.when(goes_right)(lambda: to_near(part, r, 1, "wait_send"))


def solution(mesh):
    G, B, N = mesh.shape["grp"], mesh.shape["blk"], mesh.shape["set"]

    def per_device(queries, keys, values, valid, offsets, w_out):
        rows, width = queries.shape
        plan = Plan(G, B, N, rows)
        vmem = pl.BlockSpec(memory_space=pltpu.VMEM)
        smem = pl.BlockSpec(memory_space=pltpu.SMEM)
        dma = pltpu.SemaphoreType.DMA
        ra, rb, rc = plan.sizes
        attention = pl.pallas_call(
            functools.partial(kernel, plan),
            out_shape=jax.ShapeDtypeStruct((rows, width), jnp.bfloat16),
            in_specs=[vmem, vmem, vmem, vmem, smem],
            out_specs=vmem,
            scratch_shapes=[
                pltpu.VMEM((G, B, N, 2 * CHUNKS + 1, ra, LANES), jnp.bfloat16),
                pltpu.VMEM((B, N, 2 * CHUNKS, rb, LANES), jnp.bfloat16),
                pltpu.VMEM((N, 2 * CHUNKS, rc, LANES), jnp.bfloat16),
                pltpu.VMEM((CHUNKS, plan.total, LANES), jnp.bfloat16),
                pltpu.VMEM((plan.total, LANES), jnp.bfloat16),
                pltpu.VMEM((3, CHUNKS + 1, plan.total, LANES), jnp.float32),
                pltpu.VMEM((3, CHUNKS + 1, plan.total, LANES), jnp.float32),
                pltpu.VMEM((CHUNKS, plan.total, LANES), jnp.bfloat16),
                pltpu.VMEM((plan.total, LANES), jnp.bfloat16),
                dma((3, N)),
                dma((3, N, 2)),
                dma((2, B, N)),
                dma((2, B, N)),
                dma((G, B, N)),
                dma((G // 2, B, N)),
                dma((G, B, N)),
                dma((2,)),
                dma((2,)),
            ],
            compiler_params=pltpu.CompilerParams(
                collective_id=0, has_side_effects=True, vmem_limit_bytes=60 * 1024 * 1024
            ),
        )(queries, keys, values, valid.reshape(1, rows), offsets)
        return jnp.dot(attention, w_out, preferred_element_type=jnp.float32).astype(jnp.bfloat16)

    rows_spec = P(("grp", "blk", "set"), None)
    return jax.shard_map(
        per_device,
        mesh=mesh,
        in_specs=(rows_spec, rows_spec, rows_spec, P(("grp", "blk", "set")), P(), P()),
        out_specs=rows_spec,
        check_vma=False,
    )
```
